8 devices in a mesh: dp: 1 (over z), row: 2 (over y), col: 4 (over x, core).
Axes of the slice: x: 2, y: 2, z: 1, core: 2. Of those that a mesh axis runs over, the one named last changes fastest.
Arguments:
- x: bfloat16 [2, 8, 1024, 2048], P(None, ('dp', 'row', 'col'))
- idx: int32 [2, 8, 1024, 6], P(None, ('dp', 'row', 'col'))
- gates: float32 [2, 8, 1024, 6], P(None, ('dp', 'row', 'col'))
- wq: bfloat16 [2048, 2048], replicated
- wk: bfloat16 [2048, 2048], replicated
- wv: bfloat16 [2048, 2048], replicated
- wo: bfloat16 [2048, 2048], replicated
- gattn: float32 [2048], replicated
- gmoe: float32 [2048], replicated
- w1: bfloat16 [64, 2048, 1408], P(('row', 'col'))
- w3: bfloat16 [64, 2048, 1408], P(('row', 'col'))
- w2: bfloat16 [64, 1408, 2048], P(('row', 'col'))
Outputs:
- output: bfloat16 [2, 8, 1024, 2048], P(None, ('dp', 'row', 'col'))
All inputs are finite; a program needn't handle non-finite values.
Results may differ from the reference program's by a relative error of at most 0.00860727.
Values are sent between devices in bfloat16 or wider.
A program may use at most 1 GiB of HBM per device.

```python
import jax
import jax.numpy as jnp
from jax import lax

D = 2048
HEADS = 16
HEAD = 128
EXPERTS = 64
TOP = 6
FF = 1408
TOKENS = 1024
SEQ = 1024
GROUP = 8

CAP = ((TOP * ((2 * TOKENS + EXPERTS - 1) // EXPERTS) + 7) // 8) * 8
NTOK = GROUP * TOKENS
NSEQ = NTOK // SEQ


def draw_routing(key):
    k1, k2, k3 = jax.random.split(key, 3)
    k1 = jax.random.fold_in(k1, 7919)
    k2 = jax.random.fold_in(k2, 7919)
    offset = jax.random.randint(k1, (), 0, EXPERTS)
    ranks = jax.vmap(lambda kk: jax.random.permutation(kk, TOKENS))(jax.random.split(k2, GROUP))
    half = TOKENS // 2
    quarter = EXPERTS // 4
    r = jnp.where(ranks < half, (ranks * quarter) // half, quarter + ((ranks - half) * (EXPERTS - quarter)) // half)
    pos = (offset + r[:, :, None] - jnp.arange(TOP)[None, None, :]) % EXPERTS
    idx = pos.reshape(NSEQ, SEQ, TOP).astype(jnp.int32)
    gates = jax.nn.softmax(jax.random.normal(k3, (NSEQ, SEQ, TOP), jnp.float32), axis=-1)
    return idx, gates


def setup_inputs(seed: int = 0, part: int = 0) -> dict:
    key = jax.random.key(seed)
    kw = jax.random.split(key, 10)
    kp = jax.random.split(jax.random.fold_in(key, part), 4)
    hd = HEADS * HEAD
    base = jax.random.normal(kp[0], (2, NSEQ, SEQ, D), jnp.float32)
    shift = 0.8 * jax.random.normal(kp[1], (2, NSEQ, 1, D), jnp.float32)
    x = (base + shift).astype(jnp.bfloat16)
    ia, ga = draw_routing(kp[2])
    ib, gb = draw_routing(kp[3])
    idx = jnp.stack([ia, ib])
    gates = jnp.stack([ga, gb])
    wq = (jax.random.normal(kw[0], (D, hd), jnp.float32) * D ** -0.5).astype(jnp.bfloat16)
    wk = (jax.random.normal(kw[1], (D, hd), jnp.float32) * D ** -0.5).astype(jnp.bfloat16)
    wv = (jax.random.normal(kw[2], (D, hd), jnp.float32) * D ** -0.5).astype(jnp.bfloat16)
    wo = (jax.random.normal(kw[3], (hd, D), jnp.float32) * hd ** -0.5).astype(jnp.bfloat16)
    gattn = 1.0 + 0.3 * jax.random.normal(kw[4], (D,), jnp.float32)
    gmoe = 1.0 + 0.3 * jax.random.normal(kw[5], (D,), jnp.float32)
    w1 = (jax.random.normal(kw[6], (EXPERTS, D, FF), jnp.float32) * D ** -0.5).astype(jnp.bfloat16)
    w3 = (jax.random.normal(kw[7], (EXPERTS, D, FF), jnp.float32) * D ** -0.5).astype(jnp.bfloat16)
    w2 = (jax.random.normal(kw[8], (EXPERTS, FF, D), jnp.float32) * 2.0 * FF ** -0.5).astype(jnp.bfloat16)
    return {"x": x, "idx": idx, "gates": gates, "wq": wq, "wk": wk, "wv": wv, "wo": wo, "gattn": gattn, "gmoe": gmoe, "w1": w1, "w3": w3, "w2": w2}


def rms(v, g):
    vf = v.astype(jnp.float32)
    return (vf * lax.rsqrt(jnp.mean(vf * vf, axis=-1, keepdims=True) + 1e-6) * g).astype(jnp.bfloat16)


def attention(x, wq, wk, wv, wo, gattn):
    u = rms(x, gattn)

    def proj(w):
        a = jnp.dot(u, w, preferred_element_type=jnp.float32).astype(jnp.bfloat16)
        return a.reshape(NSEQ, SEQ, HEADS, HEAD).transpose(2, 0, 1, 3)

    q, k, v = proj(wq), proj(wk), proj(wv)
    causal = jnp.arange(SEQ)[:, None] >= jnp.arange(SEQ)[None, :]

    def one_head(qkv):
        qh, kh, vh = qkv
        s = jnp.einsum("cre,cle->crl", qh.astype(jnp.float32), kh.astype(jnp.float32)) * HEAD ** -0.5
        s = jnp.where(causal[None], s, -1e30)
        p = jax.nn.softmax(s, axis=-1).astype(jnp.bfloat16)
        o = jnp.einsum("crl,cle->cre", p.astype(jnp.float32), vh.astype(jnp.float32))
        return o.astype(jnp.bfloat16)

    o = lax.map(one_head, (q, k, v))
    o = o.transpose(1, 2, 0, 3).reshape(NTOK, HEADS * HEAD)
    a = jnp.dot(o, wo, preferred_element_type=jnp.float32)
    return (x.astype(jnp.float32) + a).astype(jnp.bfloat16)


def moe(h, idx, gates, w1, w3, w2, gmoe):
    z = rms(h, gmoe)
    zpad = jnp.concatenate([z, jnp.zeros((1, D), jnp.bfloat16)], axis=0)
    flat = idx.reshape(-1)
    gflat = gates.reshape(-1)
    order = jnp.argsort(flat, stable=True)
    counts = jnp.zeros((EXPERTS,), jnp.int32).at[flat].add(1)
    starts = jnp.cumsum(counts) - counts
    width = GROUP * CAP

    def step(acc, per_expert):
        a1, a3, a2, st, ct = per_expert
        slot = st + jnp.arange(width)
        valid = slot < st + ct
        pair = order[jnp.minimum(slot, NTOK * TOP - 1)]
        tok = jnp.where(valid, pair // TOP, NTOK)
        gate = jnp.where(valid, gflat[pair], 0.0)
        rows = zpad[tok]
        h1 = jnp.dot(rows, a1, preferred_element_type=jnp.float32)
        h3 = jnp.dot(rows, a3, preferred_element_type=jnp.float32)
        act = (jax.nn.silu(h1) * h3).astype(jnp.bfloat16)
        out = jnp.dot(act, a2, preferred_element_type=jnp.float32).astype(jnp.bfloat16)
        acc = acc.at[tok].add(gate[:, None] * out.astype(jnp.float32), mode="drop")
        return acc, None

    acc, _ = lax.scan(step, jnp.zeros((NTOK, D), jnp.float32), (w1, w3, w2, starts, counts))
    return (h.astype(jnp.float32) + acc).astype(jnp.bfloat16)


def reference(x, idx, gates, wq, wk, wv, wo, gattn, gmoe, w1, w3, w2):
    ys = []
    for m in range(2):
        h = attention(x[m].reshape(NTOK, D), wq, wk, wv, wo, gattn)
        y = moe(h, idx[m].reshape(NTOK, TOP), gates[m].reshape(NTOK, TOP), w1, w3, w2, gmoe)
        ys.append(y.reshape(NSEQ, SEQ, D))
    return jnp.stack(ys)
```

```python
import functools

import jax
import jax.numpy as jnp
from jax import lax
from jax.experimental import pallas as pl
from jax.experimental.pallas import tpu as pltpu
from jax.sharding import PartitionSpec as P

HEAD = 128
LANE = 128
TM = 384
SUB = 128
PIECE = 64
DEPTH = 4
CHUNKS = ((3, 3, 2), (4, 4))
UN = 8
QB = 256
VMEM = 63 * 1024 * 1024


def rms(v, g):
    vf = v.astype(jnp.float32)
    return (vf * lax.rsqrt(jnp.mean(vf * vf, axis=-1, keepdims=True) + 1e-6) * g).astype(jnp.bfloat16)


def capacity(t, top, n_exp):
    return ((top * ((2 * t + n_exp - 1) // n_exp) + 7) // 8) * 8


def flash_body(q_ref, k_ref, v_ref, o_ref):
    seq = q_ref.shape[0]
    qb = min(QB, seq)
    causal = lax.broadcasted_iota(jnp.int32, (qb, qb), 0) >= lax.broadcasted_iota(jnp.int32, (qb, qb), 1)
    for i in range(seq // qb):
        q = q_ref[i * qb:(i + 1) * qb, :]
        n = (i + 1) * qb
        s = lax.dot_general(q, k_ref[:n, :], (((1,), (1,)), ((), ())), preferred_element_type=jnp.float32)
        s = s * HEAD ** -0.5
        diag = jnp.where(causal, s[:, i * qb:], -1e30)
        s = diag if i == 0 else jnp.concatenate([s[:, :i * qb], diag], axis=1)
        e = jnp.exp(s - jnp.max(s, axis=1, keepdims=True))
        p = (e * (1.0 / jnp.sum(e, axis=1, keepdims=True))).astype(jnp.bfloat16)
        o = jnp.dot(p, v_ref[:n, :], preferred_element_type=jnp.float32)
        o_ref[i * qb:(i + 1) * qb, :] = o.astype(jnp.bfloat16)


def flash(q, k, v, seq):
    t, width = q.shape
    spec = pl.BlockSpec((seq, HEAD), lambda b, h: (b, h))
    return pl.pallas_call(
        flash_body,
        grid=(t // seq, width // HEAD),
        in_specs=[spec] * 3,
        out_specs=spec,
        out_shape=jax.ShapeDtypeStruct(q.shape, jnp.bfloat16),
        compiler_params=pltpu.CompilerParams(vmem_limit_bytes=VMEM),
        cost_estimate=pl.CostEstimate(flops=3 * t * seq * width, bytes_accessed=8 * t * width, transcendentals=t * seq * width // HEAD),
        name="flash",
    )(q, k, v)


def attention(x, wq, wk, wv, wo, g):
    ns, seq, d = x.shape
    xf = x.reshape(ns * seq, d)
    u = rms(xf, g)

    def proj(w):
        return jnp.dot(u, w, preferred_element_type=jnp.float32).astype(jnp.bfloat16)

    o = flash(proj(wq), proj(wk), proj(wv), seq)
    a = jnp.dot(o, wo, preferred_element_type=jnp.float32)
    return (xf.astype(jnp.float32) + a).astype(jnp.bfloat16)


def source_plan(idx, gates, chunk_of, n_chunk, n_exp):
    t, top = idx.shape
    slot = chunk_of[:, None] * n_exp + idx
    key = (slot * t + jnp.arange(t, dtype=jnp.int32)[:, None]).reshape(-1)
    cnt = jnp.sum((slot[:, :, None] == jnp.arange(n_chunk * n_exp, dtype=idx.dtype)).astype(jnp.float32), axis=(0, 1))
    return key, gates.reshape(-1), cnt


def device_plan(tok, gates, cnt, me, el, rows):
    ep, pairs = tok.shape
    off = jnp.cumsum(cnt, axis=1) - cnt
    pick = lambda a: lax.dynamic_slice(a, (0, me * el), (ep, el)).T
    c = pick(cnt)
    seg_list = pick(off) + jnp.arange(ep, dtype=jnp.int32)[None, :] * pairs
    ce = jnp.sum(c, axis=1)
    tiles = (ce + TM - 1) // TM
    tile0 = jnp.cumsum(tiles) - tiles
    used = jnp.sum(tiles)
    i = jnp.arange(rows // TM, dtype=jnp.int32)
    i = jnp.minimum(i, jnp.maximum(used - 1, 0))
    te = jnp.sum((i[:, None] >= (tile0 + tiles)[None, :]).astype(jnp.int32), axis=1)
    te = jnp.minimum(te, el - 1)
    onehot = te[:, None] == jnp.arange(el, dtype=jnp.int32)[None, :]
    at = lambda a: jnp.sum(jnp.where(onehot, a[None, :], 0), axis=1)
    r0 = (i - at(tile0)) * TM
    before = jnp.cumsum(c, axis=1) - c
    pad = lambda a: jnp.pad(a.reshape(-1), (0, 2 * UN))
    i32 = lambda a: a.astype(jnp.int32).reshape(-1)
    return dict(tok=pad(tok), gates=pad(gates), te=i32(te), r0=i32(r0), tn=i32(at(ce) - r0), used=i32(used), before=i32(before),
                seg_list=i32(seg_list), seg_row=i32(tile0[:, None] * TM + before), seg_cnt=i32(c))


def dispatch_body(ep, used, te, r0s, before, seg_list, seg_cnt, tok, z_hbm, x_ref, z_vm, rows, sem):
    i = pl.program_id(0)
    tc = z_vm.shape[0] // ep
    sub = z_vm.shape[1]
    pitch = sub + 1

    @pl.when(i == 0)
    def _():
        cp = pltpu.make_async_copy(z_hbm, z_vm, sem)
        cp.start()
        cp.wait()

    @pl.when(i < used[0])
    def _():
        e = te[i]
        r0 = r0s[i]
        for s in range(ep):
            seg = e * ep + s
            first = before[seg] - r0
            lo = jnp.maximum(first, 0)
            hi = jnp.minimum(first + seg_cnt[seg], TM)
            base = seg_list[seg] - first

            def step(k, _):
                j = lo + k * UN
                new = [z_vm[s * tc + tok[base + j + q]].astype(jnp.float32) for q in range(UN)]
                for q in range(UN):
                    rows[pl.ds((j + q) * pitch, sub), :] = new[q]
                return 0

            lax.fori_loop(0, (jnp.maximum(hi - lo, 0) + UN - 1) // UN, step, 0)
        for c in range(sub):
            x_ref[:, c * LANE:(c + 1) * LANE] = rows[pl.ds(c, TM, stride=pitch), :].astype(jnp.bfloat16)


def last_used(i, used):
    return jnp.minimum(i, jnp.maximum(used[0] - 1, 0))


def dispatch(plan, z3, ep, rows):
    n, sub, _ = z3.shape
    d = sub * LANE
    return pl.pallas_call(
        functools.partial(dispatch_body, ep),
        grid_spec=pltpu.PrefetchScalarGridSpec(
            num_scalar_prefetch=7,
            grid=(rows // TM,),
            in_specs=[pl.BlockSpec(memory_space=pl.ANY)],
            out_specs=pl.BlockSpec((TM, d), lambda i, used, *_: (last_used(i, used), 0)),
            scratch_shapes=[pltpu.VMEM((n, sub, LANE), jnp.bfloat16), pltpu.VMEM(((TM + UN) * (sub + 1), LANE), jnp.float32), pltpu.SemaphoreType.DMA],
        ),
        out_shape=jax.ShapeDtypeStruct((rows, d), jnp.bfloat16),
        compiler_params=pltpu.CompilerParams(vmem_limit_bytes=VMEM, dimension_semantics=("arbitrary",)),
        cost_estimate=pl.CostEstimate(flops=rows * d * 16, bytes_accessed=4 * rows * d, transcendentals=0),
        name="dispatch",
    )(plan["used"], plan["te"], plan["r0"], plan["before"], plan["seg_list"], plan["seg_cnt"], plan["tok"], z3)


def expert_body(used, te, tn, x_ref, w1_ref, w3_ref, w2_ref, o_ref, tail, mid, out):
    i = pl.program_id(0)
    ff = w1_ref.shape[2]
    d = w2_ref.shape[2]
    sub = d // LANE
    pitch = sub + 1
    head = ff // 256 * 256
    rest = ff - head
    step = 256
    dot = functools.partial(jnp.dot, preferred_element_type=jnp.float32)

    def act(h1, h3):
        return (jax.nn.silu(h1) * h3).astype(jnp.bfloat16)

    def run(n):
        x = x_ref[:n]
        for lo in range(0, head, step):
            mid[:n, lo:lo + step] = act(dot(x, w1_ref[0, :, lo:lo + step]), dot(x, w3_ref[0, :, lo:lo + step]))
        if rest:
            ht = dot(x, tail[...])
            mid[:n, head:] = act(ht[:, :rest], ht[:, rest:])
        for lo in range(0, d, step):
            o = dot(mid[:n], w2_ref[0, :, lo:lo + step])
            for c in range(step // LANE):
                out[pl.ds(lo // LANE + c, n, stride=pitch), :] = o[:, c * LANE:(c + 1) * LANE]

        def pack(k, _):
            new = [out[pl.ds((k * 16 + q) * pitch, sub), :].astype(jnp.bfloat16) for q in range(16)]
            for q in range(16):
                o_ref[k * 16 + q] = new[q]
            return 0

        lax.fori_loop(0, n // 16, pack, 0)

    @pl.when(i < used[0])
    def _():
        if rest:
            @pl.when((i == 0) | (te[i] != te[jnp.maximum(i - 1, 0)]))
            def _():
                tail[:, :rest] = w1_ref[0, :, head:]
                tail[:, rest:] = w3_ref[0, :, head:]

        for n in range(SUB, TM + 1, SUB):
            lo = n - SUB if n > SUB else -1
            hi = n if n < TM else 1 << 30

            @pl.when((tn[i] > lo) & (tn[i] <= hi))
            def _(n=n):
                run(n)


def experts(plan, x, w1, w3, w2, spare):
    rows, d = x.shape
    el, _, ff = w1.shape
    sub = d // LANE

    def weight(a, b):
        return pl.BlockSpec((1, a, b), lambda i, used, te, tn: (te[i], 0, 0))

    return pl.pallas_call(
        expert_body,
        grid_spec=pltpu.PrefetchScalarGridSpec(
            num_scalar_prefetch=3,
            grid=(rows // TM,),
            in_specs=[pl.BlockSpec((TM, d), lambda i, used, te, tn: (last_used(i, used), 0)), weight(d, ff), weight(d, ff), weight(ff, d)],
            out_specs=pl.BlockSpec((TM, sub, LANE), lambda i, used, te, tn: (last_used(i, used), 0, 0)),
            scratch_shapes=[pltpu.VMEM((d, 2 * (ff % 256) or 256), jnp.bfloat16), pltpu.VMEM((TM, ff), jnp.bfloat16), pltpu.VMEM((TM * (sub + 1), LANE), jnp.float32)],
        ),
        out_shape=jax.ShapeDtypeStruct((rows + spare, sub, LANE), jnp.bfloat16),
        compiler_params=pltpu.CompilerParams(vmem_limit_bytes=VMEM, dimension_semantics=("arbitrary",)),
        cost_estimate=pl.CostEstimate(flops=3 * rows * d * ff, bytes_accessed=4 * rows * d + 6 * el * d * ff, transcendentals=rows * ff),
        name="experts",
    )(plan["used"], plan["te"], plan["tn"], x, w1, w3, w2)


def partial_body(ep, el, cap, seg_list, seg_row, seg_cnt, tok, gates, rows_hbm, p_ref, buf, sem):
    e = pl.program_id(1)
    n = pl.program_id(0) * el + e

    def copies(n, act):
        seg = (n % el) * ep + n // el
        for k in range(0, cap, PIECE):
            @pl.when(seg_cnt[seg] > k)
            def _(k=k):
                at = pl.ds(seg_row[seg] + k, PIECE)
                act(pltpu.make_async_copy(rows_hbm.at[at], buf.at[n % DEPTH, pl.ds(k, PIECE)], sem.at[n % DEPTH, k // PIECE]))

    @pl.when(n == 0)
    def _():
        for k in range(DEPTH - 1):
            copies(n + k, lambda c: c.start())

    @pl.when(n + DEPTH - 1 < ep * el)
    def _():
        copies(n + DEPTH - 1, lambda c: c.start())

    @pl.when(e == 0)
    def _():
        p_ref[...] = jnp.zeros_like(p_ref)

    copies(n, lambda c: c.wait())
    seg = e * ep + n // el
    cnt = seg_cnt[seg]
    base = seg_list[seg]
    rows = buf.at[n % DEPTH]

    def add(j, un):
        at = [tok[base + j + q] for q in range(un)]
        new = [p_ref[at[q]] + gates[base + j + q] * rows[j + q].astype(jnp.float32) for q in range(un)]
        for q in range(un):
            p_ref[at[q]] = new[q]

    full = cnt // UN

    def step(r, _):
        add(r * UN, UN)
        return 0

    lax.fori_loop(0, full, step, 0)

    def one(j, _):
        add(j, 1)
        return 0

    lax.fori_loop(full * UN, cnt, one, 0)


def partial_sums(plan, rows, ep, el, cap, tc):
    _, sub, _ = rows.shape
    cap = (cap + PIECE - 1) // PIECE * PIECE
    return pl.pallas_call(
        functools.partial(partial_body, ep, el, cap),
        grid_spec=pltpu.PrefetchScalarGridSpec(
            num_scalar_prefetch=5,
            grid=(ep, el),
            in_specs=[pl.BlockSpec(memory_space=pl.ANY)],
            out_specs=pl.BlockSpec((tc, sub, LANE), lambda s, e, *_: (s, 0, 0)),
            scratch_shapes=[pltpu.VMEM((DEPTH, cap, sub, LANE), jnp.bfloat16), pltpu.SemaphoreType.DMA((DEPTH, cap // PIECE))],
        ),
        out_shape=jax.ShapeDtypeStruct((ep * tc, sub, LANE), jnp.float32),
        compiler_params=pltpu.CompilerParams(vmem_limit_bytes=VMEM, dimension_semantics=("arbitrary", "arbitrary")),
        cost_estimate=pl.CostEstimate(flops=rows.size * 2, bytes_accessed=rows.size * 4, transcendentals=0),
        name="partial_sums",
    )(plan["seg_list"], plan["seg_row"], plan["seg_cnt"], plan["tok"], plan["gates"], rows)


def final_body(a_ref, h_ref, *refs):
    y_ref = refs[-1]
    for k in range(a_ref.shape[1]):
        cols = slice(k * LANE, (k + 1) * LANE)
        y_ref[:, cols] = (h_ref[:, cols].astype(jnp.float32) + a_ref[:, k, :]).astype(jnp.bfloat16)


def final_sum(acc, h, first, y, at, total):
    tc, sub, _ = acc.shape
    d = sub * LANE
    specs = [pl.BlockSpec((SUB, sub, LANE), lambda i: (i, 0, 0)), pl.BlockSpec((SUB, d), lambda i: (first // SUB + i, 0))]
    extra = []
    if y is not None:
        specs.append(pl.BlockSpec(memory_space=pl.ANY))
        extra.append(y)
    return pl.pallas_call(
        final_body,
        grid=(tc // SUB,),
        in_specs=specs,
        out_specs=pl.BlockSpec((SUB, d), lambda i: (at // SUB + i, 0)),
        out_shape=jax.ShapeDtypeStruct((total, d), jnp.bfloat16),
        input_output_aliases={2: 0} if extra else {},
        compiler_params=pltpu.CompilerParams(vmem_limit_bytes=VMEM),
        cost_estimate=pl.CostEstimate(flops=2 * tc * d, bytes_accessed=8 * tc * d, transcendentals=0),
        name="final_sum",
    )(acc, h, *extra)


def after(a, *deps):
    return lax.optimization_barrier((a,) + deps)[0]


def solution(mesh):
    ep_axes = ("row", "col")
    tok_axes = ("dp", "row", "col")
    ep = mesh.shape["row"] * mesh.shape["col"]

    def local(x, idx, gates, wq, wk, wv, wo, gattn, gmoe, w1, w3, w2):
        nm, ns, seq, d = x.shape
        t = ns * seq
        top = idx.shape[-1]
        el = w1.shape[0]
        n_exp = el * ep
        sub = d // LANE
        me = lax.axis_index(ep_axes).astype(jnp.int32)
        chunks = []
        for m in range(nm):
            first = 0
            for place, part in enumerate(CHUNKS[m]):
                chunks.append((m, first, part * t // 8, place))
                first += part * t // 8
        n_chunk = max(len(c) for c in CHUNKS)

        hs, zs = [], []
        xm = x[0]
        for m in range(nm):
            h = attention(xm, wq, wk, wv, wo, gattn)
            z = rms(h, gmoe).reshape(t, sub, LANE)
            hs.append(h)
            zs += [lax.all_gather(z[a:a + n], ep_axes, axis=0, tiled=True) for k, a, n, _ in chunks if k == m]
            if m == 0:
                idx, gates = after((idx, gates), z)
                keys, gs, cnts = [], [], []
                for k in range(nm):
                    chunk_of = jnp.zeros((t,), jnp.int32)
                    for kk, a, n, _ in chunks:
                        if kk == k and a > 0:
                            chunk_of = chunk_of + (jnp.arange(t) >= a).astype(jnp.int32)
                    key, g, cnt = source_plan(idx[k].reshape(t, top), gates[k].reshape(t, top), chunk_of, n_chunk, n_exp)
                    keys.append(key)
                    gs.append(g)
                    cnts.append(cnt)
                key, g = lax.sort((jnp.stack(keys), jnp.stack(gs)), dimension=1, num_keys=1)
                pack = jnp.concatenate([(key % t).astype(jnp.float32), g, jnp.stack(cnts)], axis=1)
                allp = lax.all_gather(pack, ep_axes, axis=0)
            if m + 1 < nm:
                xm = after(x[m + 1], z)
        ints = allp.astype(jnp.int32)
        pairs = t * top
        plans, rows, caps = [], [], []
        for m, a, n, place in chunks:
            cap = min(capacity(t, top, n_exp), n)
            span = slice(a * top, (a + n) * top)
            c0 = 2 * pairs + place * n_exp
            r = el * ((ep * cap + TM - 1) // TM) * TM
            plans.append(device_plan(ints[:, m, span] - a, allp[:, m, pairs:2 * pairs][:, span], ints[:, m, c0:c0 + n_exp], me, el, r))
            rows.append(r)
            caps.append(cap)

        accs = []
        xr = dispatch(plans[0], zs[0], ep, rows[0])
        for q, (m, a, n, _) in enumerate(chunks):
            out = experts(plans[q], xr, w1, w3, w2, PIECE)
            part = partial_sums(plans[q], out, ep, el, caps[q], n)
            accs.append(lax.psum_scatter(part, ep_axes, scatter_dimension=0, tiled=True))
            if q + 1 < len(chunks):
                xr = dispatch(plans[q + 1], after(zs[q + 1], part), ep, rows[q + 1])
        y = None
        for q, (m, a, n, _) in enumerate(chunks):
            y = final_sum(accs[q], hs[m], a, y, m * t + a, nm * t)
        return y.reshape(nm, ns, seq, d)

    tok_spec = P(None, tok_axes)
    exp_spec = P(ep_axes)
    return jax.shard_map(local, mesh=mesh,
                         in_specs=(tok_spec, tok_spec, tok_spec, P(), P(), P(), P(), P(), P(), exp_spec, exp_spec, exp_spec),
                         out_specs=tok_spec, check_vma=False)
```

```python
import functools

import jax
import jax.numpy as jnp
from jax import lax
from jax.experimental import pallas as pl
from jax.experimental.pallas import tpu as pltpu
from jax.sharding import PartitionSpec as P

HEAD = 128
LANE = 128
TM = 448
SIZES = (128, 256, 320, 384, 448)
SUB = 128
PIECE = 64
DEPTH = 4
CHUNKS = ((4, 2, 2), (4, 2, 2))
UN = 8
QB = 256
VMEM = 63 * 1024 * 1024


def rms(v, g):
    vf = v.astype(jnp.float32)
    return (vf * lax.rsqrt(jnp.mean(vf * vf, axis=-1, keepdims=True) + 1e-6) * g).astype(jnp.bfloat16)


def capacity(t, top, n_exp):
    return ((top * ((2 * t + n_exp - 1) // n_exp) + 7) // 8) * 8


def flash_body(q_ref, k_ref, v_ref, o_ref):
    seq = q_ref.shape[0]
    qb = min(QB, seq)
    causal = lax.broadcasted_iota(jnp.int32, (qb, qb), 0) >= lax.broadcasted_iota(jnp.int32, (qb, qb), 1)
    for i in range(seq // qb):
        q = q_ref[i * qb:(i + 1) * qb, :]
        n = (i + 1) * qb
        s = lax.dot_general(q, k_ref[:n, :], (((1,), (1,)), ((), ())), preferred_element_type=jnp.float32)
        s = s * HEAD ** -0.5
        diag = jnp.where(causal, s[:, i * qb:], -1e30)
        s = diag if i == 0 else jnp.concatenate([s[:, :i * qb], diag], axis=1)
        e = jnp.exp(s - jnp.max(s, axis=1, keepdims=True))
        p = (e * (1.0 / jnp.sum(e, axis=1, keepdims=True))).astype(jnp.bfloat16)
        o = jnp.dot(p, v_ref[:n, :], preferred_element_type=jnp.float32)
        o_ref[i * qb:(i + 1) * qb, :] = o.astype(jnp.bfloat16)


def flash(q, k, v, seq):
    t, width = q.shape
    spec = pl.BlockSpec((seq, HEAD), lambda b, h: (b, h))
    return pl.pallas_call(
        flash_body,
        grid=(t // seq, width // HEAD),
        in_specs=[spec] * 3,
        out_specs=spec,
        out_shape=jax.ShapeDtypeStruct(q.shape, jnp.bfloat16),
        compiler_params=pltpu.CompilerParams(vmem_limit_bytes=VMEM),
        cost_estimate=pl.CostEstimate(flops=3 * t * seq * width, bytes_accessed=8 * t * width, transcendentals=t * seq * width // HEAD),
        name="flash",
    )(q, k, v)


def attention(x, wq, wk, wv, wo, g):
    ns, seq, d = x.shape
    xf = x.reshape(ns * seq, d)
    u = rms(xf, g)

    def proj(w):
        return jnp.dot(u, w, preferred_element_type=jnp.float32).astype(jnp.bfloat16)

    o = flash(proj(wq), proj(wk), proj(wv), seq)
    a = jnp.dot(o, wo, preferred_element_type=jnp.float32)
    return (xf.astype(jnp.float32) + a).astype(jnp.bfloat16)


def source_plan(idx, gates, chunk_of, n_chunk, n_exp):
    t, top = idx.shape
    slot = chunk_of[:, None] * n_exp + idx
    key = (slot * t + jnp.arange(t, dtype=jnp.int32)[:, None]).reshape(-1)
    cnt = jnp.sum((slot[:, :, None] == jnp.arange(n_chunk * n_exp, dtype=idx.dtype)).astype(jnp.float32), axis=(0, 1))
    return key, gates.reshape(-1), cnt


def device_plans(cnt, pairs, me, el, nt):
    nq, ep, _ = cnt.shape
    off = jnp.cumsum(cnt, axis=2) - cnt
    pick = lambda a: lax.dynamic_slice(a, (0, 0, me * el), (nq, ep, el)).transpose(0, 2, 1)
    c = pick(cnt)
    seg_list = pick(off) + (jnp.array(pairs, jnp.int32)[:, None] * jnp.arange(ep, dtype=jnp.int32)[None, :])[:, None, :]
    before = jnp.cumsum(c, axis=2) - c
    ce = jnp.sum(c, axis=2)
    tiles = (ce + TM - 1) // TM
    tile1 = jnp.cumsum(tiles, axis=1)
    tile0 = tile1 - tiles
    used = tile1[:, -1]
    i = jnp.minimum(jnp.arange(nt, dtype=jnp.int32)[None, :], jnp.maximum(used - 1, 0)[:, None])
    te = jnp.minimum(jnp.sum((i[:, :, None] >= tile1[:, None, :]).astype(jnp.int32), axis=2), el - 1)
    ids = jnp.arange(el, dtype=jnp.int32)
    onehot = te[:, :, None] == ids
    at = lambda a: jnp.sum(jnp.where(onehot, a[:, None, :], 0), axis=2)
    r0 = (i - at(tile0)) * TM
    active = (tiles > 0).astype(jnp.int32)
    place = jnp.cumsum(active, axis=1) - active
    later = jnp.where((ids[None, None, :] > ids[None, :, None]) & (tiles > 0)[:, None, :], ids[None, None, :], el)
    nxt = jnp.min(later, axis=2)
    i32 = lambda a: a.astype(jnp.int32).reshape(-1)
    return dict(te=i32(te), r0=i32(r0), tn=i32(at(ce) - r0), used=i32(used), slot=i32(at(place) % 2), nxt=i32(at(nxt)),
                before=i32(before), seg_list=i32(seg_list), seg_row=i32(tile0[:, :, None] * TM + before), seg_cnt=i32(c))


def dispatch_body(ep, el, q0, nt, used, te, r0s, before, seg_list, seg_cnt, tok, z_hbm, x_ref, z_vm, rows, sem):
    i = pl.program_id(0)
    tc = z_vm.shape[0] // ep
    sub = z_vm.shape[1]
    pitch = sub + 1

    @pl.when(i == 0)
    def _():
        cp = pltpu.make_async_copy(z_hbm, z_vm, sem)
        cp.start()
        cp.wait()

    @pl.when(i < used[q0])
    def _():
        e = te[q0 * nt + i]
        r0 = r0s[q0 * nt + i]
        for s in range(ep):
            seg = (q0 * el + e) * ep + s
            first = before[seg] - r0
            lo = jnp.maximum(first, 0)
            hi = jnp.minimum(first + seg_cnt[seg], TM)
            base = seg_list[seg] - first

            def step(k, _):
                j = lo + k * UN
                new = [z_vm[s * tc + tok[base + j + q]].astype(jnp.float32) for q in range(UN)]
                for q in range(UN):
                    rows[pl.ds((j + q) * pitch, sub), :] = new[q]
                return 0

            lax.fori_loop(0, (jnp.maximum(hi - lo, 0) + UN - 1) // UN, step, 0)
        for c in range(sub):
            x_ref[:, c * LANE:(c + 1) * LANE] = rows[pl.ds(c, TM, stride=pitch), :].astype(jnp.bfloat16)


def last_used(i, used, q):
    return jnp.minimum(i, jnp.maximum(used[q] - 1, 0))


def dispatch(plan, tok, q, z3, ep, el, rows):
    n, sub, _ = z3.shape
    d = sub * LANE
    return pl.pallas_call(
        functools.partial(dispatch_body, ep, el, q, rows // TM),
        grid_spec=pltpu.PrefetchScalarGridSpec(
            num_scalar_prefetch=7,
            grid=(rows // TM,),
            in_specs=[pl.BlockSpec(memory_space=pl.ANY)],
            out_specs=pl.BlockSpec((TM, d), lambda i, used, *_: (last_used(i, used, q), 0)),
            scratch_shapes=[pltpu.VMEM((n, sub, LANE), jnp.bfloat16), pltpu.VMEM(((TM + UN) * (sub + 1), LANE), jnp.float32), pltpu.SemaphoreType.DMA],
        ),
        out_shape=jax.ShapeDtypeStruct((rows, d), jnp.bfloat16),
        compiler_params=pltpu.CompilerParams(vmem_limit_bytes=VMEM, dimension_semantics=("arbitrary",)),
        cost_estimate=pl.CostEstimate(flops=rows * d * 16, bytes_accessed=4 * rows * d, transcendentals=0),
        name="dispatch",
    )(plan["used"], plan["te"], plan["r0"], plan["before"], plan["seg_list"], plan["seg_cnt"], tok, z3)


def expert_body(el, q, nt, used, te, tn, slot, nxt, x_ref, w1_hbm, w3_hbm, w2_hbm, o_ref, w1_ref, w3_ref, w2_ref, tail, mid, out, sem):
    i = pl.program_id(0)
    at = q * nt + i
    k = slot[at]
    ff = w1_ref.shape[2]
    d = w2_ref.shape[2]

    def weights(e, k):
        pieces = ((w1_hbm, w1_ref), (w3_hbm, w3_ref), (w2_hbm, w2_ref))
        return [pltpu.make_async_copy(a.at[e], b.at[k], sem.at[k, n]) for n, (a, b) in enumerate(pieces)]

    sub = d // LANE
    pitch = sub + 1
    head = ff // 256 * 256
    rest = ff - head
    step = 256
    dot = functools.partial(jnp.dot, preferred_element_type=jnp.float32)

    def act(h1, h3):
        return (jax.nn.silu(h1) * h3).astype(jnp.bfloat16)

    def run(n):
        x = x_ref[:n]
        for lo in range(0, head, step):
            mid[:n, lo:lo + step] = act(dot(x, w1_ref[k, :, lo:lo + step]), dot(x, w3_ref[k, :, lo:lo + step]))
        if rest:
            ht = dot(x, tail[...])
            mid[:n, head:] = act(ht[:, :rest], ht[:, rest:])
        for lo in range(0, d, step):
            o = dot(mid[:n], w2_ref[k, :, lo:lo + step])
            for c in range(step // LANE):
                out[pl.ds(lo // LANE + c, n, stride=pitch), :] = o[:, c * LANE:(c + 1) * LANE]

        def pack(j, _):
            new = [out[pl.ds((j * 16 + r) * pitch, sub), :].astype(jnp.bfloat16) for r in range(16)]
            for r in range(16):
                o_ref[j * 16 + r] = new[r]
            return 0

        lax.fori_loop(0, n // 16, pack, 0)

    @pl.when(i < used[q])
    def _():
        @pl.when((i == 0) | (te[at] != te[jnp.maximum(at - 1, 0)]))
        def _():
            @pl.when(i == 0)
            def _():
                for c in weights(te[at], k):
                    c.start()

            for c in weights(te[at], k):
                c.wait()

            @pl.when(nxt[at] < el)
            def _():
                for c in weights(nxt[at], 1 - k):
                    c.start()

            if rest:
                tail[:, :rest] = w1_ref[k, :, head:]
                tail[:, rest:] = w3_ref[k, :, head:]

        for j, n in enumerate(SIZES):
            lo = SIZES[j - 1] if j else -1
            hi = n if n < TM else 1 << 30

            @pl.when((tn[at] > lo) & (tn[at] <= hi))
            def _(n=n):
                run(n)


def experts(plan, q, x, w1, w3, w2, spare):
    rows, d = x.shape
    el, _, ff = w1.shape
    sub = d // LANE

    return pl.pallas_call(
        functools.partial(expert_body, el, q, rows // TM),
        grid_spec=pltpu.PrefetchScalarGridSpec(
            num_scalar_prefetch=5,
            grid=(rows // TM,),
            in_specs=[pl.BlockSpec((TM, d), lambda i, used, *_: (last_used(i, used, q), 0))] + [pl.BlockSpec(memory_space=pl.ANY)] * 3,
            out_specs=pl.BlockSpec((TM, sub, LANE), lambda i, used, *_: (last_used(i, used, q), 0, 0)),
            scratch_shapes=[pltpu.VMEM((2, d, ff), jnp.bfloat16), pltpu.VMEM((2, d, ff), jnp.bfloat16), pltpu.VMEM((2, ff, d), jnp.bfloat16),
                            pltpu.VMEM((d, 2 * (ff % 256) or 256), jnp.bfloat16), pltpu.VMEM((TM, ff), jnp.bfloat16), pltpu.VMEM((TM * (sub + 1), LANE), jnp.float32),
                            pltpu.SemaphoreType.DMA((2, 3))],
        ),
        out_shape=jax.ShapeDtypeStruct((rows + spare, sub, LANE), jnp.bfloat16),
        compiler_params=pltpu.CompilerParams(vmem_limit_bytes=VMEM, dimension_semantics=("arbitrary",)),
        cost_estimate=pl.CostEstimate(flops=3 * rows * d * ff, bytes_accessed=4 * rows * d + 6 * el * d * ff, transcendentals=rows * ff),
        name="experts",
    )(plan["used"], plan["te"], plan["tn"], plan["slot"], plan["nxt"], x, w1, w3, w2)


def partial_body(ep, el, cap, q0, seg_list, seg_row, seg_cnt, tok, gates, rows_hbm, p_ref, buf, sem):
    e = pl.program_id(1)
    n = pl.program_id(0) * el + e

    def copies(n, act):
        seg = (q0 * el + n % el) * ep + n // el
        for k in range(0, cap, PIECE):
            @pl.when(seg_cnt[seg] > k)
            def _(k=k):
                at = pl.ds(seg_row[seg] + k, PIECE)
                act(pltpu.make_async_copy(rows_hbm.at[at], buf.at[n % DEPTH, pl.ds(k, PIECE)], sem.at[n % DEPTH, k // PIECE]))

    @pl.when(n == 0)
    def _():
        for k in range(DEPTH - 1):
            copies(n + k, lambda c: c.start())

    @pl.when(n + DEPTH - 1 < ep * el)
    def _():
        copies(n + DEPTH - 1, lambda c: c.start())

    @pl.when(e == 0)
    def _():
        p_ref[...] = jnp.zeros_like(p_ref)

    copies(n, lambda c: c.wait())
    seg = (q0 * el + e) * ep + n // el
    cnt = seg_cnt[seg]
    base = seg_list[seg]
    rows = buf.at[n % DEPTH]

    def add(j, un):
        at = [tok[base + j + q] for q in range(un)]
        new = [p_ref[at[q]] + gates[base + j + q] * rows[j + q].astype(jnp.float32) for q in range(un)]
        for q in range(un):
            p_ref[at[q]] = new[q]

    full = cnt // UN

    def step(r, _):
        add(r * UN, UN)
        return 0

    lax.fori_loop(0, full, step, 0)

    def one(j, _):
        add(j, 1)
        return 0

    lax.fori_loop(full * UN, cnt, one, 0)


def partial_sums(plan, tok, gates, q, rows, ep, el, cap, tc):
    _, sub, _ = rows.shape
    cap = (cap + PIECE - 1) // PIECE * PIECE
    return pl.pallas_call(
        functools.partial(partial_body, ep, el, cap, q),
        grid_spec=pltpu.PrefetchScalarGridSpec(
            num_scalar_prefetch=5,
            grid=(ep, el),
            in_specs=[pl.BlockSpec(memory_space=pl.ANY)],
            out_specs=pl.BlockSpec((tc, sub, LANE), lambda s, e, *_: (s, 0, 0)),
            scratch_shapes=[pltpu.VMEM((DEPTH, cap, sub, LANE), jnp.bfloat16), pltpu.SemaphoreType.DMA((DEPTH, cap // PIECE))],
        ),
        out_shape=jax.ShapeDtypeStruct((ep * tc, sub, LANE), jnp.float32),
        compiler_params=pltpu.CompilerParams(vmem_limit_bytes=VMEM, dimension_semantics=("arbitrary", "arbitrary")),
        cost_estimate=pl.CostEstimate(flops=rows.size * 2, bytes_accessed=rows.size * 4, transcendentals=0),
        name="partial_sums",
    )(plan["seg_list"], plan["seg_row"], plan["seg_cnt"], tok, gates, rows)


def final_body(a_ref, h_ref, *refs):
    y_ref = refs[-1]
    for k in range(a_ref.shape[1]):
        cols = slice(k * LANE, (k + 1) * LANE)
        y_ref[:, cols] = (h_ref[:, cols].astype(jnp.float32) + a_ref[:, k, :]).astype(jnp.bfloat16)


def final_sum(acc, h, first, y, at, total):
    tc, sub, _ = acc.shape
    d = sub * LANE
    specs = [pl.BlockSpec((SUB, sub, LANE), lambda i: (i, 0, 0)), pl.BlockSpec((SUB, d), lambda i: (first // SUB + i, 0))]
    extra = []
    if y is not None:
        specs.append(pl.BlockSpec(memory_space=pl.ANY))
        extra.append(y)
    return pl.pallas_call(
        final_body,
        grid=(tc // SUB,),
        in_specs=specs,
        out_specs=pl.BlockSpec((SUB, d), lambda i: (at // SUB + i, 0)),
        out_shape=jax.ShapeDtypeStruct((total, d), jnp.bfloat16),
        input_output_aliases={2: 0} if extra else {},
        compiler_params=pltpu.CompilerParams(vmem_limit_bytes=VMEM),
        cost_estimate=pl.CostEstimate(flops=2 * tc * d, bytes_accessed=8 * tc * d, transcendentals=0),
        name="final_sum",
    )(acc, h, *extra)


def after(a, *deps):
    return lax.optimization_barrier((a,) + deps)[0]


def solution(mesh):
    ep_axes = ("row", "col")
    tok_axes = ("dp", "row", "col")
    ep = mesh.shape["row"] * mesh.shape["col"]

    def local(x, idx, gates, wq, wk, wv, wo, gattn, gmoe, w1, w3, w2):
        nm, ns, seq, d = x.shape
        t = ns * seq
        top = idx.shape[-1]
        el = w1.shape[0]
        n_exp = el * ep
        sub = d // LANE
        me = lax.axis_index(ep_axes).astype(jnp.int32)
        chunks = []
        for m in range(nm):
            first = 0
            for place, part in enumerate(CHUNKS[m]):
                chunks.append((m, first, part * t // 8, place))
                first += part * t // 8
        n_chunk = max(len(c) for c in CHUNKS)

        hs, zs = [], []
        xm = x[0]
        for m in range(nm):
            h = attention(xm, wq, wk, wv, wo, gattn)
            z = rms(h, gmoe).reshape(t, sub, LANE)
            hs.append(h)
            zs += [lax.all_gather(z[a:a + n], ep_axes, axis=0, tiled=True) for k, a, n, _ in chunks if k == m]
            if m == 0:
                idx, gates = after((idx, gates), z)
                keys, gs, cnts = [], [], []
                for k in range(nm):
                    chunk_of = jnp.zeros((t,), jnp.int32)
                    for kk, a, n, _ in chunks:
                        if kk == k and a > 0:
                            chunk_of = chunk_of + (jnp.arange(t) >= a).astype(jnp.int32)
                    key, g, cnt = source_plan(idx[k].reshape(t, top), gates[k].reshape(t, top), chunk_of, n_chunk, n_exp)
                    keys.append(key)
                    gs.append(g)
                    cnts.append(cnt)
                key, g = lax.sort((jnp.stack(keys), jnp.stack(gs)), dimension=1, num_keys=1)
                pack = jnp.concatenate([(key % t).astype(jnp.float32), g, jnp.stack(cnts)], axis=1)
                allp = lax.all_gather(pack, ep_axes, axis=0)
            if m + 1 < nm:
                xm = after(x[m + 1], z)
        ints = allp.astype(jnp.int32)
        pairs = t * top
        cap = capacity(t, top, n_exp)
        rows = el * ((ep * cap + TM - 1) // TM) * TM
        pad = lambda v: jnp.pad(v.reshape(-1), (0, 2 * UN))
        toks, gate, cnt = [], [], []
        for m, a, n, place in chunks:
            span = slice(a * top, (a + n) * top)
            c0 = 2 * pairs + place * n_exp
            toks.append(pad(ints[:, m, span] - a))
            gate.append(pad(allp[:, m, pairs:2 * pairs][:, span]))
            cnt.append(ints[:, m, c0:c0 + n_exp])
        plan = device_plans(jnp.stack(cnt), [n * top for _, _, n, _ in chunks], me, el, rows // TM)

        accs = []
        xr = dispatch(plan, toks[0], 0, zs[0], ep, el, rows)
        for q, (m, a, n, _) in enumerate(chunks):
            out = experts(plan, q, xr, w1, w3, w2, PIECE)
            part = partial_sums(plan, toks[q], gate[q], q, out, ep, el, min(cap, n), n)
            accs.append(lax.psum_scatter(part, ep_axes, scatter_dimension=0, tiled=True))
            if q + 1 < len(chunks):
                xr = dispatch(plan, toks[q + 1], q + 1, after(zs[q + 1], part), ep, el, rows)
        y = None
        for q, (m, a, n, _) in enumerate(chunks):
            y = final_sum(accs[q], hs[m], a, y, m * t + a, nm * t)
        return y.reshape(nm, ns, seq, d)

    tok_spec = P(None, tok_axes)
    exp_spec = P(ep_axes)
    return jax.shard_map(local, mesh=mesh,
                         in_specs=(tok_spec, tok_spec, tok_spec, P(), P(), P(), P(), P(), P(), exp_spec, exp_spec, exp_spec),
                         out_specs=tok_spec, check_vma=False)
```
